32 devices in a mesh: grp: 4 (over z), dev: 8 (over y, x, core).
Axes of the slice: x: 2, y: 2, z: 4, core: 2. Of those that a mesh axis runs over, the one named last changes fastest.
Arguments:
- qkv_weight: bfloat16 [2, 4608, 8192], P(None, ('grp', 'dev')), may hold values from -0.09375 to 0.09375
- gate_up_weight: bfloat16 [2, 4608, 73728], P(None, ('grp', 'dev')), may hold values from -0.09375 to 0.09375
- head_slot: int32 [64], replicated, may hold values from 0 to 63, each once
- layer_ids: int32 [2], replicated, may hold values from 0 to 45
- stored_qkv: int32 [46, 64], replicated, may hold values from -16384 to 16383
- stored_gate_up: int32 [46, 576], replicated, may hold values from -16384 to 16383
Outputs:
- served_qkv: bfloat16 [2, 4608, 8192], P(None, 'grp', 'dev')
- served_gate_up: bfloat16 [2, 4608, 73728], P(None, 'grp', 'dev')
- qkv_mismatch: float32 [2, 64], P(None, 'dev')
- gate_up_mismatch: float32 [2, 576], P(None, 'dev')
The draws below stay inside these ranges and needn't reach their ends.
Inputs may be any that keep to these rules, and one draw needn't show every extreme that they name: `head_slot`: each of the 64 heads appears once.
All inputs are finite; a program needn't handle non-finite values.
Results may differ from the reference program's by a relative error of at most 0.0004.
Values may be sent and summed in bfloat16 or wider, within the bound.
A program may use at most 256 MiB of HBM per device.

```python
import jax
import jax.numpy as jnp
from jax import lax

D = 4608
HEAD_DIM = 128
FF = 36864
STORED = 46
LAYERS = 2
BLK = 128
NHEAD = 64
N_DEV = 8


def touch_ends(values, key, low, largest):
    place = [jax.random.randint(jax.random.fold_in(key, axis), (), 0, length) for axis, length in enumerate(values.shape)]
    longest = values.shape.index(max(values.shape))
    next_to = place[:longest] + [(place[longest] + 1) % values.shape[longest]] + place[longest + 1:]
    return values.at[tuple(place)].set(low).at[tuple(next_to)].set(largest)


def steps_of(rng, shape, split, smallest, high):
    factor_of, own = 1.0, jax.random.fold_in(rng, 6)
    for axis_at, shards_of in split:
        draws = jnp.exp(jax.random.uniform(jax.random.fold_in(own, axis_at), (shards_of,), jnp.float32, smallest / len(split), high / len(split)))
        factor_of = factor_of * jnp.repeat(draws, shape[axis_at] // shards_of).reshape([-1 if axis == axis_at else 1 for axis in range(len(shape))])
    return factor_of


def centred(key, dims, spread, bound, split=(), dtype=jnp.bfloat16):
    factor_of = steps_of(key, dims, split, -0.22, 0.18) if split else 1.0
    values = jax.random.normal(key, dims, jnp.float32) * spread * factor_of
    return jnp.minimum(jnp.maximum(values, -bound), bound).astype(dtype)


def setup_inputs(seed: int = 0) -> dict:
    key_of = jax.random.split(jax.random.key(seed), 7)
    return {
        "qkv_weight": centred(key_of[0], (LAYERS, D, NHEAD * HEAD_DIM), D ** -0.5, 0.09375, ((1, 32),)),
        "gate_up_weight": centred(key_of[1], (LAYERS, D, 2 * FF), D ** -0.5, 0.09375, ((1, 32),)),
        "head_slot": jax.random.permutation(key_of[2], NHEAD).astype(jnp.int32),
        "layer_ids": jax.random.randint(key_of[3], (LAYERS,), 0, STORED).astype(jnp.int32),
        "stored_qkv": touch_ends(jax.random.randint(key_of[4], (STORED, NHEAD), -16384, 16384), jax.random.fold_in(key_of[4], 1), -16384, 16383).astype(jnp.int32),
        "stored_gate_up": touch_ends(jax.random.randint(key_of[5], (STORED, 2 * FF // BLK), -16384, 16384), jax.random.fold_in(key_of[5], 1), -16384, 16383).astype(jnp.int32),
    }


stored_unit = 1.0 / 1024.0


def reference(qkv_weight, gate_up_weight, head_slot, layer_ids, stored_qkv, stored_gate_up):
    width = FF // N_DEV
    served_qkv = qkv_weight.reshape(LAYERS, D, NHEAD, HEAD_DIM)[:, :, head_slot, :].reshape(LAYERS, D, NHEAD * HEAD_DIM)
    served_gate_up = gate_up_weight.reshape(LAYERS, D, 2, N_DEV, width).transpose(0, 1, 3, 2, 4).reshape(LAYERS, D, 2 * FF)

    def layer_sums(pair):
        qkv_layer, gate_layer = pair
        head_sum = jnp.sum(qkv_layer.astype(jnp.float32).reshape(D, NHEAD, HEAD_DIM), axis=(0, 2))
        block_sum = jnp.sum(gate_layer.astype(jnp.float32).reshape(D, 2 * FF // BLK, BLK), axis=(0, 2))
        return head_sum, block_sum

    head_sum, block_sum = lax.map(layer_sums, (served_qkv, served_gate_up))
    picked_qkv = stored_qkv[layer_ids][:, head_slot].astype(jnp.float32)
    picked_gate = stored_gate_up[layer_ids].reshape(LAYERS, 2, N_DEV, width // BLK)
    picked_gate = picked_gate.transpose(0, 2, 1, 3).reshape(LAYERS, 2 * FF // BLK).astype(jnp.float32)
    qkv_mismatch = head_sum - picked_qkv * stored_unit
    gate_up_mismatch = block_sum - picked_gate * stored_unit
    return served_qkv, served_gate_up, qkv_mismatch, gate_up_mismatch
```

```python
import functools

import jax
import jax.numpy as jnp
from jax import lax
from jax.experimental import pallas as pl
from jax.experimental.pallas import tpu as pltpu
from jax.sharding import PartitionSpec as P

HEAD_DIM = 128
BLK = 128
MESH = pl.DeviceIdType.MESH

stored_unit = 1.0 / 1024.0


def partner(me, k, n):
    out = 0
    bit = 1
    while bit < n:
        mine = lax.rem(lax.div(me, bit), 2)
        out = out + bit * ((1 - mine) if k & bit else mine)
        bit *= 2
    return out


def exchange_kernel(
    groups, owners,
    slot_ref, gate_ref, qkv_ref,
    held_ref, perm_ref, tot_ref,
    own_buf, chunk_buf, q_in, q_out, colsum, part, parts_z, mine_z, parts_d,
    send_sem, recv_sem, own_sem, out_sem, chunk_sem, q_sem, zs_sem, zr_sem, ds_sem, dr_sem,
):
    me = lax.axis_index("dev")
    grp = lax.axis_index("grp")
    layers, rows, total = gate_ref.shape
    ff = total // 2
    width = ff // owners
    blocks = width // BLK
    heads = qkv_ref.shape[2] // HEAD_DIM
    slots = heads // owners

    barrier = pltpu.get_barrier_semaphore()
    for k in range(1, owners):
        pl.semaphore_signal(barrier, inc=1, device_id={"dev": partner(me, k, owners)}, device_id_type=MESH)
    for j in range(1, groups):
        pl.semaphore_signal(barrier, inc=1, device_id={"grp": lax.rem(grp + j, groups)}, device_id_type=MESH)
    pl.semaphore_wait(barrier, owners - 1 + groups - 1)

    def columns(p, owner):
        return pl.ds(pl.multiple_of(p * ff + owner * width, BLK), width)

    def send(k, l, p):
        to = partner(me, k, owners)
        return pltpu.make_async_remote_copy(
            src_ref=gate_ref.at[l, :, columns(p, to)],
            dst_ref=held_ref.at[me, l, :, pl.ds(p * width, width)],
            send_sem=send_sem.at[k, l, p],
            recv_sem=recv_sem.at[k, l, p],
            device_id={"dev": to},
            device_id_type=MESH,
        )

    hops = {k: bin(k >> 1).count("1") for k in range(1, owners)}
    near = sorted((k for k in hops if hops[k] == 1), key=lambda k: (k & 1, k))
    far = sorted((k for k in hops if hops[k] > 1), key=lambda k: (hops[k], k & 1, k))
    cores = [k for k in hops if hops[k] == 0]
    pieces = [(l, p) for l in range(layers) for p in range(2)]
    for l, p in pieces:
        for k in near:
            send(k, l, p).start()
    for l, p in pieces:
        for k in cores:
            send(k, l, p).start()

    own_in = [
        pltpu.make_async_copy(gate_ref.at[l, :, columns(p, me)], own_buf.at[l * 2 + p], own_sem.at[l * 2 + p])
        for l, p in pieces
    ]
    own_out = [
        pltpu.make_async_copy(
            own_buf.at[l * 2 + p], held_ref.at[me, l, :, pl.ds(p * width, width)], out_sem.at[l * 2 + p]
        )
        for l, p in pieces
    ]
    q_store = pltpu.make_async_copy(q_out, perm_ref, q_sem.at[heads])

    def q_load(h):
        source = qkv_ref.at[:, :, pl.ds(pl.multiple_of(h * HEAD_DIM, HEAD_DIM), HEAD_DIM)]
        return pltpu.make_async_copy(source, q_in.at[h], q_sem.at[h])

    def q_start(h, carry):
        q_load(h).start()
        return carry

    def q_wait(h, carry):
        q_load(h).wait()
        return carry
    for copy in own_in:
        copy.start()
    lax.fori_loop(0, heads, q_start, 0)

    per = 2 * layers
    count = owners * per

    def chunk(i, slot):
        owner = i // per
        l = (i % per) // 2
        p = i % 2
        return pltpu.make_async_copy(gate_ref.at[l, :, columns(p, owner)], chunk_buf.at[slot], chunk_sem.at[slot])

    chunk(0, 0).start()
    for copy in own_in:
        copy.wait()
    for copy in own_out:
        copy.start()

    colsum[...] = jnp.zeros_like(colsum)
    part[...] = jnp.zeros_like(part)
    lax.fori_loop(0, heads, q_wait, 0)
    lane8 = lax.broadcasted_iota(jnp.int32, (8, BLK), 1)
    row8 = lax.broadcasted_iota(jnp.int32, (8, BLK), 0)

    def head_step(s, carry):
        owner = s // slots
        j = s % slots
        head = q_in[slot_ref[s]]
        for l in range(layers):
            values = head[l]
            q_out[owner, l, :, pl.ds(pl.multiple_of(j * HEAD_DIM, HEAD_DIM), HEAD_DIM)] = values
            cols = jnp.sum(values.astype(jnp.float32), axis=0, keepdims=True)
            head_sum = jnp.sum(cols, axis=1, keepdims=True)
            here = (lane8 == j) & (row8 == per + l)
            part[owner] += jnp.where(here, jnp.broadcast_to(head_sum, (8, BLK)), 0.0)
        return carry

    lax.fori_loop(0, heads, head_step, 0)

    def sum_step(i, carry):
        slot = i % 2

        @pl.when(i + 1 < count)
        def _():
            chunk(i + 1, (i + 1) % 2).start()

        chunk(i, slot).wait()
        sums = jnp.sum(chunk_buf[slot].astype(jnp.float32), axis=0, keepdims=True)
        colsum[i // per, pl.ds(i % per, 1), :] = sums
        return carry

    lax.fori_loop(0, count, sum_step, 0)

    def block_step(o, carry):
        acc = part[o]
        for b in range(blocks):
            s = jnp.sum(colsum[o, :, b * BLK:(b + 1) * BLK], axis=1, keepdims=True)
            acc = acc + jnp.where(lane8 == b, jnp.broadcast_to(s, (8, BLK)), 0.0)
        part[o] = acc
        return carry

    lax.fori_loop(0, owners, block_step, 0)
    q_store.start()

    across = [
        pltpu.make_async_remote_copy(
            src_ref=part,
            dst_ref=parts_z.at[j - 1],
            send_sem=zs_sem.at[j - 1],
            recv_sem=zr_sem.at[j - 1],
            device_id={"grp": lax.rem(grp + j, groups)},
            device_id_type=MESH,
        )
        for j in range(1, groups)
    ]
    for copy in across:
        copy.start()
    for copy in across:
        copy.wait()
    group_sum = part[...]
    for j in range(groups - 1):
        group_sum = group_sum + parts_z[j]
    mine_z[...] = group_sum

    for k in far:
        for l, p in pieces[:1]:
            send(k, l, p).start()
    along = []
    for k in range(1, owners):
        to = partner(me, k, owners)
        along.append(
            pltpu.make_async_remote_copy(
                src_ref=mine_z.at[to],
                dst_ref=parts_d.at[k - 1],
                send_sem=ds_sem.at[k - 1],
                recv_sem=dr_sem.at[k - 1],
                device_id={"dev": to},
                device_id_type=MESH,
            )
        )
    for copy in along:
        copy.start()
    for l, p in pieces[1:]:
        for k in far:
            send(k, l, p).start()
    for copy in along:
        copy.wait()
    all_sum = mine_z[me]
    for k in range(owners - 1):
        all_sum = all_sum + parts_d[k]
    tot_ref[...] = all_sum

    q_store.wait()
    for copy in own_out:
        copy.wait()
    for k in near + cores + far:
        for l, p in pieces:
            send(k, l, p).wait()


def exchange(head_slot, gate, qkv, groups, owners):
    layers, rows, total = gate.shape
    width = total // 2 // owners
    slots = qkv.shape[2] // HEAD_DIM // owners
    any_space = pl.BlockSpec(memory_space=pl.ANY)
    dma = pltpu.SemaphoreType.DMA
    f32 = jnp.float32
    return pl.pallas_call(
        functools.partial(exchange_kernel, groups, owners),
        name="exchange",
        out_shape=(
            jax.ShapeDtypeStruct((owners, layers, rows, 2 * width), gate.dtype),
            jax.ShapeDtypeStruct((owners, layers, rows, slots * HEAD_DIM), qkv.dtype),
            jax.ShapeDtypeStruct((8, BLK), f32),
        ),
        in_specs=[pl.BlockSpec(memory_space=pltpu.SMEM), any_space, any_space],
        out_specs=(any_space, pl.BlockSpec(memory_space=pltpu.HBM), pl.BlockSpec(memory_space=pltpu.VMEM)),
        scratch_shapes=[
            pltpu.VMEM((2 * layers, rows, width), gate.dtype),
            pltpu.VMEM((2, rows, width), gate.dtype),
            pltpu.VMEM((owners * slots, layers, rows, HEAD_DIM), qkv.dtype),
            pltpu.VMEM((owners, layers, rows, slots * HEAD_DIM), qkv.dtype),
            pltpu.VMEM((owners, 8, width), f32),
            pltpu.VMEM((owners, 8, BLK), f32),
            pltpu.VMEM((groups - 1, owners, 8, BLK), f32),
            pltpu.VMEM((owners, 8, BLK), f32),
            pltpu.VMEM((owners - 1, 8, BLK), f32),
            dma((owners, layers, 2)),
            dma((owners, layers, 2)),
            dma((2 * layers,)),
            dma((2 * layers,)),
            dma((2,)),
            dma((owners * slots + 1,)),
            dma((groups - 1,)),
            dma((groups - 1,)),
            dma((owners - 1,)),
            dma((owners - 1,)),
        ],
        compiler_params=pltpu.CompilerParams(
            collective_id=0, has_side_effects=True, vmem_limit_bytes=48 * 1024 * 1024
        ),
        cost_estimate=pl.CostEstimate(flops=0, bytes_accessed=4 * gate.size, transcendentals=0),
    )(head_slot, gate, qkv)


def place_kernel(in_ref, out_ref):
    out_ref[...] = in_ref[0]


def place(held):
    owners, layers, rows, columns = held.shape
    if rows % 16:
        return held.transpose(1, 0, 2, 3).reshape(layers, owners * rows, columns)
    return pl.pallas_call(
        place_kernel,
        name="place",
        grid=(layers, owners),
        in_specs=[pl.BlockSpec((1, 1, rows, columns), lambda l, s: (s, l, 0, 0))],
        out_specs=pl.BlockSpec((1, rows, columns), lambda l, s: (l, s, 0)),
        out_shape=jax.ShapeDtypeStruct((layers, owners * rows, columns), held.dtype),
        compiler_params=pltpu.CompilerParams(vmem_limit_bytes=40 * 1024 * 1024),
        cost_estimate=pl.CostEstimate(
            flops=0, bytes_accessed=4 * held.size, transcendentals=0
        ),
    )(held)


def body(qkv_weight, gate_up_weight, head_slot, layer_ids, stored_qkv, stored_gate_up):
    groups = lax.axis_size("grp")
    owners = lax.axis_size("dev")
    owner = lax.axis_index("dev")
    layers = qkv_weight.shape[0]
    slots = head_slot.shape[0] // owners
    blocks = gate_up_weight.shape[2] // 2 // owners // BLK
    held, perm, tot = exchange(head_slot, gate_up_weight, qkv_weight, groups, owners)
    moved = lax.all_to_all(perm, "dev", split_axis=0, concat_axis=0, tiled=True)
    served_gate = place(held)
    served_qkv = place(moved)
    block_sum = tot[: 2 * layers, :blocks].reshape(layers, 2 * blocks)
    head_sum = tot[2 * layers : 3 * layers, :slots]
    pick = (layer_ids[:, None] == jnp.arange(stored_qkv.shape[0], dtype=jnp.int32)[None, :])
    own_heads = lax.dynamic_slice_in_dim(head_slot, owner * slots, slots, 0)
    head_pick = own_heads[:, None] == jnp.arange(head_slot.shape[0], dtype=jnp.int32)[None, :]
    rows_qkv = jnp.sum(jnp.where(pick[:, :, None], stored_qkv[None], 0), axis=1)
    picked_qkv = jnp.sum(jnp.where(head_pick[None], rows_qkv[:, None, :], 0), axis=2)
    stored_split = stored_gate_up.reshape(stored_gate_up.shape[0], 2, owners * blocks)
    own_gate = lax.dynamic_slice_in_dim(stored_split, owner * blocks, blocks, 2)
    picked_gate = jnp.sum(jnp.where(pick[:, :, None, None], own_gate[None], 0), axis=1)
    picked_gate = picked_gate.reshape(layers, 2 * blocks)
    qkv_mismatch = head_sum - picked_qkv.astype(jnp.float32) * stored_unit
    gate_up_mismatch = block_sum - picked_gate.astype(jnp.float32) * stored_unit
    return (served_qkv, served_gate, qkv_mismatch, gate_up_mismatch)


def solution(mesh):
    placed = (P(None, ("grp", "dev"), None), P(None, ("grp", "dev"), None), P(), P(), P(), P())
    return jax.shard_map(
        body,
        mesh=mesh,
        in_specs=placed,
        out_specs=(P(None, "grp", "dev"), P(None, "grp", "dev"), P(None, "dev"), P(None, "dev")),
        check_vma=False,
    )
```

```python
import functools

import jax
import jax.numpy as jnp
from jax import lax
from jax.experimental import pallas as pl
from jax.experimental.pallas import tpu as pltpu
from jax.sharding import PartitionSpec as P

HEAD_DIM = 128
BLK = 128
MESH = pl.DeviceIdType.MESH

stored_unit = 1.0 / 1024.0


def partner(me, k, n):
    out = 0
    bit = 1
    while bit < n:
        mine = lax.rem(lax.div(me, bit), 2)
        out = out + bit * ((1 - mine) if k & bit else mine)
        bit *= 2
    return out


def exchange_kernel(
    groups, owners,
    slot_ref, gate_ref, qkv_ref,
    held_ref, perm_ref, tot_ref,
    own_buf, chunk_buf, q_in, q_out, colsum, part, parts_z, mine_z, parts_d,
    send_sem, recv_sem, own_sem, out_sem, chunk_sem, q_sem, zs_sem, zr_sem, ds_sem, dr_sem,
):
    me = lax.axis_index("dev")
    grp = lax.axis_index("grp")
    layers, rows, total = gate_ref.shape
    ff = total // 2
    width = ff // owners
    blocks = width // BLK
    heads = qkv_ref.shape[2] // HEAD_DIM
    slots = heads // owners

    barrier = pltpu.get_barrier_semaphore()
    for k in range(1, owners):
        pl.semaphore_signal(barrier, inc=1, device_id={"dev": partner(me, k, owners)}, device_id_type=MESH)
    for j in range(1, groups):
        pl.semaphore_signal(barrier, inc=1, device_id={"grp": lax.rem(grp + j, groups)}, device_id_type=MESH)
    pl.semaphore_wait(barrier, owners - 1 + groups - 1)

    def columns(p, owner):
        return pl.ds(pl.multiple_of(p * ff + owner * width, BLK), width)

    def send(k, l, p):
        to = partner(me, k, owners)
        return pltpu.make_async_remote_copy(
            src_ref=gate_ref.at[l, :, columns(p, to)],
            dst_ref=held_ref.at[me, l, :, pl.ds(p * width, width)],
            send_sem=send_sem.at[k, l, p],
            recv_sem=recv_sem.at[k, l, p],
            device_id={"dev": to},
            device_id_type=MESH,
        )

    hops = {k: bin(k >> 1).count("1") for k in range(1, owners)}
    near = sorted((k for k in hops if hops[k] == 1), key=lambda k: (k & 1, k))
    far = sorted((k for k in hops if hops[k] > 1), key=lambda k: (hops[k], k & 1, k))
    cores = [k for k in hops if hops[k] == 0]
    pieces = [(l, p) for l in range(layers) for p in range(2)]
    for l, p in pieces:
        for k in near:
            send(k, l, p).start()
    for l, p in pieces:
        for k in cores:
            send(k, l, p).start()

    own_in = [
        pltpu.make_async_copy(gate_ref.at[l, :, columns(p, me)], own_buf.at[l * 2 + p], own_sem.at[l * 2 + p])
        for l, p in pieces
    ]
    own_out = [
        pltpu.make_async_copy(
            own_buf.at[l * 2 + p], held_ref.at[me, l, :, pl.ds(p * width, width)], out_sem.at[l * 2 + p]
        )
        for l, p in pieces
    ]
    q_store = pltpu.make_async_copy(q_out, perm_ref, q_sem.at[heads])

    def q_load(h):
        source = qkv_ref.at[:, :, pl.ds(pl.multiple_of(h * HEAD_DIM, HEAD_DIM), HEAD_DIM)]
        return pltpu.make_async_copy(source, q_in.at[h], q_sem.at[h])

    def q_start(h, carry):
        q_load(h).start()
        return carry

    def q_wait(h, carry):
        q_load(h).wait()
        return carry
    for copy in own_in:
        copy.start()
    lax.fori_loop(0, heads, q_start, 0)

    per = 2 * layers
    count = owners * per

    def chunk(i, slot):
        owner = i // per
        l = (i % per) // 2
        p = i % 2
        return pltpu.make_async_copy(gate_ref.at[l, :, columns(p, owner)], chunk_buf.at[slot], chunk_sem.at[slot])

    chunk(0, 0).start()
    for copy in own_in:
        copy.wait()
    for copy in own_out:
        copy.start()

    colsum[...] = jnp.zeros_like(colsum)
    part[...] = jnp.zeros_like(part)
    lax.fori_loop(0, heads, q_wait, 0)
    lane8 = lax.broadcasted_iota(jnp.int32, (8, BLK), 1)
    row8 = lax.broadcasted_iota(jnp.int32, (8, BLK), 0)

    def head_step(s, carry):
        owner = s // slots
        j = s % slots
        head = q_in[slot_ref[s]]
        for l in range(layers):
            values = head[l]
            q_out[owner, l, :, pl.ds(pl.multiple_of(j * HEAD_DIM, HEAD_DIM), HEAD_DIM)] = values
            cols = jnp.sum(values.astype(jnp.float32), axis=0, keepdims=True)
            head_sum = jnp.sum(cols, axis=1, keepdims=True)
            here = (lane8 == j) & (row8 == per + l)
            part[owner] += jnp.where(here, jnp.broadcast_to(head_sum, (8, BLK)), 0.0)
        return carry

    lax.fori_loop(0, heads, head_step, 0)

    def sum_step(i, carry):
        slot = i % 2

        @pl.when(i + 1 < count)
        def _():
            chunk(i + 1, (i + 1) % 2).start()

        chunk(i, slot).wait()
        sums = jnp.sum(chunk_buf[slot].astype(jnp.float32), axis=0, keepdims=True)
        colsum[i // per, pl.ds(i % per, 1), :] = sums
        return carry

    lax.fori_loop(0, count, sum_step, 0)

    def block_step(o, carry):
        acc = part[o]
        for b in range(blocks):
            s = jnp.sum(colsum[o, :, b * BLK:(b + 1) * BLK], axis=1, keepdims=True)
            acc = acc + jnp.where(lane8 == b, jnp.broadcast_to(s, (8, BLK)), 0.0)
        part[o] = acc
        return carry

    lax.fori_loop(0, owners, block_step, 0)
    q_store.start()

    across = [
        pltpu.make_async_remote_copy(
            src_ref=part,
            dst_ref=parts_z.at[j - 1],
            send_sem=zs_sem.at[j - 1],
            recv_sem=zr_sem.at[j - 1],
            device_id={"grp": lax.rem(grp + j, groups)},
            device_id_type=MESH,
        )
        for j in range(1, groups)
    ]
    for copy in across:
        copy.start()
    for copy in across:
        copy.wait()
    group_sum = part[...]
    for j in range(groups - 1):
        group_sum = group_sum + parts_z[j]
    mine_z[...] = group_sum

    for k in far:
        for l, p in pieces[:1]:
            send(k, l, p).start()
    along = []
    for k in range(1, owners):
        to = partner(me, k, owners)
        along.append(
            pltpu.make_async_remote_copy(
                src_ref=mine_z.at[to],
                dst_ref=parts_d.at[k - 1],
                send_sem=ds_sem.at[k - 1],
                recv_sem=dr_sem.at[k - 1],
                device_id={"dev": to},
                device_id_type=MESH,
            )
        )
    for copy in along:
        copy.start()
    for l, p in pieces[1:]:
        for k in far:
            send(k, l, p).start()
    for copy in along:
        copy.wait()
    all_sum = mine_z[me]
    for k in range(owners - 1):
        all_sum = all_sum + parts_d[k]
    tot_ref[...] = all_sum

    q_store.wait()
    for copy in own_out:
        copy.wait()
    for k in near + cores + far:
        for l, p in pieces:
            send(k, l, p).wait()


def exchange(head_slot, gate, qkv, groups, owners):
    layers, rows, total = gate.shape
    width = total // 2 // owners
    slots = qkv.shape[2] // HEAD_DIM // owners
    any_space = pl.BlockSpec(memory_space=pl.ANY)
    dma = pltpu.SemaphoreType.DMA
    f32 = jnp.float32
    return pl.pallas_call(
        functools.partial(exchange_kernel, groups, owners),
        name="exchange",
        out_shape=(
            jax.ShapeDtypeStruct((owners, layers, rows, 2 * width), gate.dtype),
            jax.ShapeDtypeStruct((owners, layers, rows, slots * HEAD_DIM), qkv.dtype),
            jax.ShapeDtypeStruct((8, BLK), f32),
        ),
        in_specs=[pl.BlockSpec(memory_space=pltpu.SMEM), any_space, any_space],
        out_specs=(any_space, pl.BlockSpec(memory_space=pltpu.HBM), pl.BlockSpec(memory_space=pltpu.VMEM)),
        scratch_shapes=[
            pltpu.VMEM((2 * layers, rows, width), gate.dtype),
            pltpu.VMEM((2, rows, width), gate.dtype),
            pltpu.VMEM((owners * slots, layers, rows, HEAD_DIM), qkv.dtype),
            pltpu.VMEM((owners, layers, rows, slots * HEAD_DIM), qkv.dtype),
            pltpu.VMEM((owners, 8, width), f32),
            pltpu.VMEM((owners, 8, BLK), f32),
            pltpu.VMEM((groups - 1, owners, 8, BLK), f32),
            pltpu.VMEM((owners, 8, BLK), f32),
            pltpu.VMEM((owners - 1, 8, BLK), f32),
            dma((owners, layers, 2)),
            dma((owners, layers, 2)),
            dma((2 * layers,)),
            dma((2 * layers,)),
            dma((2,)),
            dma((owners * slots + 1,)),
            dma((groups - 1,)),
            dma((groups - 1,)),
            dma((owners - 1,)),
            dma((owners - 1,)),
        ],
        compiler_params=pltpu.CompilerParams(
            collective_id=0, has_side_effects=True, vmem_limit_bytes=62 * 1024 * 1024
        ),
        cost_estimate=pl.CostEstimate(flops=0, bytes_accessed=4 * gate.size, transcendentals=0),
    )(head_slot, gate, qkv)


def place_kernel(in_ref, out_ref):
    rows = in_ref.shape[2]
    for s in range(in_ref.shape[0]):
        out_ref[0, s * rows : (s + 1) * rows, :] = in_ref[s, 0]


def place(held):
    owners, layers, rows, columns = held.shape
    if rows % 16:
        return held.transpose(1, 0, 2, 3).reshape(layers, owners * rows, columns)
    at_once = 1
    while at_once * 2 <= owners // 2 and at_once * rows * columns < 2**19:
        at_once *= 2
    return pl.pallas_call(
        place_kernel,
        name="place",
        grid=(layers, owners // at_once),
        in_specs=[pl.BlockSpec((at_once, 1, rows, columns), lambda l, s: (s, l, 0, 0))],
        out_specs=pl.BlockSpec((1, at_once * rows, columns), lambda l, s: (l, s, 0)),
        out_shape=jax.ShapeDtypeStruct((layers, owners * rows, columns), held.dtype),
        compiler_params=pltpu.CompilerParams(vmem_limit_bytes=40 * 1024 * 1024),
        cost_estimate=pl.CostEstimate(
            flops=0, bytes_accessed=4 * held.size, transcendentals=0
        ),
    )(held)


def body(qkv_weight, gate_up_weight, head_slot, layer_ids, stored_qkv, stored_gate_up):
    groups = lax.axis_size("grp")
    owners = lax.axis_size("dev")
    owner = lax.axis_index("dev")
    layers = qkv_weight.shape[0]
    slots = head_slot.shape[0] // owners
    blocks = gate_up_weight.shape[2] // 2 // owners // BLK
    held, perm, tot = exchange(head_slot, gate_up_weight, qkv_weight, groups, owners)
    moved = lax.all_to_all(perm, "dev", split_axis=0, concat_axis=0, tiled=True)
    served_gate = place(held)
    served_qkv = place(moved)
    block_sum = tot[: 2 * layers, :blocks].reshape(layers, 2 * blocks)
    head_sum = tot[2 * layers : 3 * layers, :slots]
    pick = (layer_ids[:, None] == jnp.arange(stored_qkv.shape[0], dtype=jnp.int32)[None, :])
    own_heads = lax.dynamic_slice_in_dim(head_slot, owner * slots, slots, 0)
    head_pick = own_heads[:, None] == jnp.arange(head_slot.shape[0], dtype=jnp.int32)[None, :]
    rows_qkv = jnp.sum(jnp.where(pick[:, :, None], stored_qkv[None], 0), axis=1)
    picked_qkv = jnp.sum(jnp.where(head_pick[None], rows_qkv[:, None, :], 0), axis=2)
    stored_split = stored_gate_up.reshape(stored_gate_up.shape[0], 2, owners * blocks)
    own_gate = lax.dynamic_slice_in_dim(stored_split, owner * blocks, blocks, 2)
    picked_gate = jnp.sum(jnp.where(pick[:, :, None, None], own_gate[None], 0), axis=1)
    picked_gate = picked_gate.reshape(layers, 2 * blocks)
    qkv_mismatch = head_sum - picked_qkv.astype(jnp.float32) * stored_unit
    gate_up_mismatch = block_sum - picked_gate.astype(jnp.float32) * stored_unit
    return (served_qkv, served_gate, qkv_mismatch, gate_up_mismatch)


def solution(mesh):
    placed = (P(None, ("grp", "dev"), None), P(None, ("grp", "dev"), None), P(), P(), P(), P())
    return jax.shard_map(
        body,
        mesh=mesh,
        in_specs=placed,
        out_specs=(P(None, "grp", "dev"), P(None, "grp", "dev"), P(None, "dev"), P(None, "dev")),
        check_vma=False,
    )
```
